256 devices in a mesh: shard: 64 (over z, y, core), model: 4 (over x).
Axes of the slice: x: 4, y: 4, z: 8, core: 2. Of those that a mesh axis runs over, the one named last changes fastest.
Arguments:
- gradients: float32 [256, 128, 4096], P(None, 'shard', 'model'), may hold values from -6 to 6
- momentum: float32 [256, 128, 4096], P(None, 'shard', 'model'), may hold values from -6 to 6
- weights: float32 [256, 128, 4096], P(None, 'shard', 'model'), may hold values from -0.1875 to 0.1875
Outputs:
- new_weights: float32 [256, 128, 4096], P(None, 'shard', 'model')
- new_momentum: float32 [256, 128, 4096], P(None, 'shard', 'model')
The draws below stay inside these ranges and needn't reach their ends.
All inputs are finite; a program needn't handle non-finite values.
Results may differ from the reference program's by a relative error of at most 0.00015.
Values sent between devices are 32-bit elements; how exact they have to be, the bound alone decides.
A program may use at most 128 MiB of HBM per device.

```python
import jax
import jax.numpy as jnp
from jax import lax

SIDE = 128
WIDE = 4096
MATS = 256
ITERS = 4


def level_of(stream_key, dims, cuts, low, top_value):
    def one(position, shards_of):
        steps = jax.random.uniform(jax.random.fold_in(jax.random.fold_in(stream_key, 6), position), (shards_of,), jnp.float32, low / len(cuts), top_value / len(cuts))
        return jnp.repeat(jnp.exp(steps), dims[position] // shards_of).reshape((-1,) + (1,) * (len(dims) - position - 1))

    level = one(*cuts[0])
    for cut in cuts[1:]:
        level = level * one(*cut)
    return level


def gaussian(rng, shape, width, reach, cuts=(), held_as=jnp.bfloat16):
    result = width * jax.random.normal(rng, shape, jnp.float32)
    if cuts:
        result = result * level_of(rng, shape, cuts, -0.22, 0.18)
    return jnp.clip(result, -reach, reach).astype(held_as)


def setup_inputs(seed: int = 0) -> dict:
    key_of = jax.random.split(jax.random.key(seed), 4)
    gradients = gaussian(key_of[0], (MATS, SIDE, WIDE), 1.0, 6.0, ((1, 64), (2, 4)), jnp.float32)
    momentum = gaussian(key_of[1], (MATS, SIDE, WIDE), 1.0, 6.0, ((1, 64), (2, 4)), jnp.float32)
    weights = gaussian(key_of[2], (MATS, SIDE, WIDE), 0.03, 0.1875, ((1, 64), (2, 4)), jnp.float32)
    return {"gradients": gradients, "momentum": momentum, "weights": weights}


hold_rate = 0.8
learn_rate = 1.0

def reference(gradients, momentum, weights):
    new_momentum = hold_rate * momentum + gradients

    def orthogonal_one(stack):
        iterate = stack[None]
        iterate = iterate * lax.rsqrt(lax.optimization_barrier(jnp.sum(iterate * iterate, axis=(1, 2), keepdims=True)) + 1e-06)
        for step in range(ITERS):
            gram = jnp.einsum('mik,mjk->mij', iterate, iterate, precision=lax.Precision.HIGHEST)
            mixed = -4.775 * gram + 2.0315 * jnp.einsum('mij,mjk->mik', gram, gram, precision=lax.Precision.HIGHEST)
            iterate = 3.4445 * iterate + jnp.einsum('mij,mjk->mik', mixed, iterate, precision=lax.Precision.HIGHEST)
        return iterate[0]
    iterate = lax.map(orthogonal_one, new_momentum)
    new_weights = weights - learn_rate * iterate
    return (new_weights, new_momentum)
```

```python
import functools

import jax
import jax.numpy as jnp
from jax import lax
from jax.experimental import pallas as pl
from jax.experimental.pallas import tpu as pltpu
from jax.sharding import PartitionSpec as P

ITERS = 4
hold_rate = 0.8
learn_rate = 1.0

GROUPS = 64
COLUMNS = 4
OWNED = 4
SIDE = 128
LANES = 128
TILES = 8
PIECE = 16
DZ_ORDER = (4, 3, 5, 2, 6, 1, 7, 0)
HIGH = lax.Precision.HIGHEST


def dot(a, b, ca, cb):
    return lax.dot_general(
        a, b, (((ca,), (cb,)), ((), ())), precision=HIGH, preferred_element_type=jnp.float32
    )


def peer_of(me, dz, k):
    z, y, core = me // 8, (me // 2) % 4, me % 2
    return ((z + dz) % 8) * 8 + ((y + k // 2) % 4) * 2 + (core + k % 2) % 2


def kernel(moved_ref, back_ref, land, res, parts, f_send, f_recv, g_send, g_recv, b_send, b_recv):
    me = lax.axis_index("shard")
    col = lax.axis_index("model")

    def at(peer):
        return (peer, col)

    barrier = pltpu.get_barrier_semaphore()

    def greet(k, _):
        pl.semaphore_signal(barrier, inc=1, device_id=at((me + k) % GROUPS), device_id_type=pl.DeviceIdType.MESH)
        return 0

    lax.fori_loop(1, GROUPS, greet, 0)
    for d in range(1, COLUMNS):
        pl.semaphore_signal(
            barrier, inc=1, device_id=(me, (col + d) % COLUMNS), device_id_type=pl.DeviceIdType.MESH
        )
    pl.semaphore_wait(barrier, GROUPS - 1 + COLUMNS - 1)

    mine = pl.multiple_of(me * PIECE, PIECE)

    def send_rows(m):
        for dz in DZ_ORDER:
            def one(k, _, dz=dz):
                peer = peer_of(me, dz, k)
                pltpu.make_async_remote_copy(
                    src_ref=moved_ref.at[peer * OWNED + m],
                    dst_ref=land.at[m, pl.ds(mine, PIECE), :],
                    send_sem=f_send.at[m],
                    recv_sem=f_recv.at[m],
                    device_id=at(peer),
                    device_id_type=pl.DeviceIdType.MESH,
                ).start()
                return 0
            lax.fori_loop(1 if dz == 0 else 0, 8, one, 0)

    for m in range(OWNED):
        send_rows(m)
    for m in range(OWNED):
        land[m, pl.ds(mine, PIECE), :] = moved_ref[me * OWNED + m]

    def tile_pair(m, j):
        sides = []
        for q in (2 * j, 2 * j + 1):
            sides.append(
                jnp.concatenate(
                    [land[m, pl.ds(2 * q + r, GROUPS, stride=PIECE), :] for r in (0, 1)], axis=0
                )
            )
        return jnp.concatenate(sides, axis=1)

    def wait_bytes(ref, sem):
        pltpu.make_async_copy(ref, ref, sem).wait()

    rows = lax.broadcasted_iota(jnp.int32, (SIDE, SIDE), 0)
    cols = lax.broadcasted_iota(jnp.int32, (SIDE, SIDE), 1)
    eye = jnp.where(rows == cols, 1.0, 0.0).astype(jnp.float32)

    def gram(m):
        wait_bytes(land.at[m, pl.ds(0, (GROUPS - 1) * PIECE), :], f_recv.at[m])
        total = None
        for j in range(TILES // 2):
            x = tile_pair(m, j)
            term = dot(x, x, 1, 1)
            total = term if total is None else total + term
        parts[m, col] = total
        for d in range(1, COLUMNS):
            pltpu.make_async_remote_copy(
                src_ref=parts.at[m, col],
                dst_ref=parts.at[m, col],
                send_sem=g_send.at[m],
                recv_sem=g_recv.at[m],
                device_id=(me, (col + d) % COLUMNS),
                device_id_type=pl.DeviceIdType.MESH,
            ).start()

    def finish(m):
        wait_bytes(parts.at[m, pl.ds(0, COLUMNS - 1)], g_recv.at[m])
        whole = (parts[m, 0] + parts[m, 1]) + (parts[m, 2] + parts[m, 3])
        power = jnp.sum(jnp.sum(whole * eye, axis=1, keepdims=True), axis=0, keepdims=True)
        scale = lax.rsqrt(power + 1e-06)
        a = whole * (scale * scale)
        product = None
        for step in range(ITERS):
            mixed = 3.4445 * eye - 4.775 * a + 2.0315 * dot(a, a, 1, 0)
            product = mixed if product is None else dot(mixed, product, 1, 0)
            if step < ITERS - 1:
                a = dot(dot(mixed, a, 1, 0), mixed, 1, 0)
        product = product * scale
        for j in range(TILES // 2):
            y = dot(product, tile_pair(m, j), 1, 0)
            for i in (0, 1):
                q = 2 * j + i
                for r in (0, 1):
                    res[m, pl.ds(2 * q + r, GROUPS, stride=PIECE), :] = y[
                        GROUPS * r : GROUPS * (r + 1), LANES * i : LANES * (i + 1)
                    ]
        for dz in DZ_ORDER:
            def one(k, _, dz=dz):
                peer = peer_of(me, dz, k)
                pltpu.make_async_remote_copy(
                    src_ref=res.at[m, pl.ds(pl.multiple_of(peer * PIECE, PIECE), PIECE), :],
                    dst_ref=back_ref.at[me * OWNED + m],
                    send_sem=b_send.at[m],
                    recv_sem=b_recv,
                    device_id=at(peer),
                    device_id_type=pl.DeviceIdType.MESH,
                ).start()
                return 0
            lax.fori_loop(1 if dz == 0 else 0, 8, one, 0)
        back_ref[me * OWNED + m] = res[m, pl.ds(mine, PIECE), :]

    gram(0)
    for m in range(OWNED):
        if m + 1 < OWNED:
            pass
        finish(m)
        if m + 1 < OWNED:
            gram(m + 1)

    for m in range(OWNED):
        wait_bytes(land.at[m, pl.ds(0, (GROUPS - 1) * PIECE), :], f_send.at[m])
        wait_bytes(parts.at[m, pl.ds(0, COLUMNS - 1)], g_send.at[m])
        wait_bytes(res.at[m, pl.ds(0, (GROUPS - 1) * PIECE), :], b_send.at[m])
    wait_bytes(back_ref.at[pl.ds(0, (GROUPS - 1) * OWNED)], b_recv)


def exchange(pieces):
    return pl.pallas_call(
        kernel,
        out_shape=jax.ShapeDtypeStruct(pieces.shape, jnp.float32),
        in_specs=[pl.BlockSpec(memory_space=pltpu.VMEM)],
        out_specs=pl.BlockSpec(memory_space=pltpu.VMEM),
        scratch_shapes=[
            pltpu.VMEM((OWNED, GROUPS * PIECE, LANES), jnp.float32),
            pltpu.VMEM((OWNED, GROUPS * PIECE, LANES), jnp.float32),
            pltpu.VMEM((OWNED, COLUMNS, SIDE, SIDE), jnp.float32),
            pltpu.SemaphoreType.DMA((OWNED,)),
            pltpu.SemaphoreType.DMA((OWNED,)),
            pltpu.SemaphoreType.DMA((OWNED,)),
            pltpu.SemaphoreType.DMA((OWNED,)),
            pltpu.SemaphoreType.DMA((OWNED,)),
            pltpu.SemaphoreType.DMA,
        ],
        compiler_params=pltpu.CompilerParams(
            collective_id=0, has_side_effects=True, vmem_limit_bytes=24 * 1024 * 1024
        ),
    )(pieces)


def to_pieces(block):
    mats = block.shape[0]
    return block.reshape(mats, 2, TILES, LANES).transpose(0, 2, 1, 3).reshape(mats, PIECE, LANES)


def from_pieces(pieces):
    mats = pieces.shape[0]
    return pieces.reshape(mats, TILES, 2, LANES).transpose(0, 2, 1, 3).reshape(mats, 2, TILES * LANES)


def on_device(gradients, momentum, weights):
    new_momentum = hold_rate * momentum + gradients
    back = from_pieces(exchange(to_pieces(new_momentum)))
    new_weights = weights - learn_rate * back
    return (new_weights, new_momentum)


def solution(mesh):
    placed = (P(None, "shard", "model"), P(None, "shard", "model"), P(None, "shard", "model"))
    return jax.shard_map(
        on_device,
        mesh=mesh,
        in_specs=placed,
        out_specs=(P(None, "shard", "model"), P(None, "shard", "model")),
        check_vma=False,
    )
```

```python
import functools

import jax
import jax.numpy as jnp
from jax import lax
from jax.experimental import pallas as pl
from jax.experimental.pallas import tpu as pltpu
from jax.sharding import PartitionSpec as P

ITERS = 4
hold_rate = 0.8
learn_rate = 1.0

GROUPS = 64
COLUMNS = 4
OWNED = 4
SIDE = 128
LANES = 128
TILES = 8
PIECE = 16
DZ_ORDER = (4, 3, 5, 2, 6, 1, 7, 0)
NEAR = [(dz, k) for dz in DZ_ORDER[:-1] for k in (0, 1)] + [(0, k) for k in (4, 5, 2, 3, 6, 7, 1)]
EARLY = 2
HIGH = lax.Precision.HIGHEST


def dot(a, b, ca, cb):
    return lax.dot_general(
        a, b, (((ca,), (cb,)), ((), ())), precision=HIGH, preferred_element_type=jnp.float32
    )


def peer_of(me, dz, k):
    z, y, core = me // 8, (me // 2) % 4, me % 2
    return ((z + dz) % 8) * 8 + ((y + k // 2) % 4) * 2 + (core + k % 2) % 2


def kernel(
    grad_ref, mom_ref, weight_ref, new_weight_ref, moved_ref,
    grad, mom, weight, land, res, parts, back,
    ready, in_sem, w_sem, f_send, f_recv, g_send, g_recv, b_send, b_recv,
):
    me = lax.axis_index("shard")
    col = lax.axis_index("model")

    def at(peer):
        return (peer, col)

    z = me // 8
    loads = []
    for i, dz in enumerate(DZ_ORDER):
        block = pl.ds(((z + dz) % 8) * 8, 8)
        for j, (ref, buf) in enumerate(((grad_ref, grad), (mom_ref, mom))):
            copy = pltpu.make_async_copy(ref.at[block], buf.at[block], in_sem.at[2 * i + j])
            copy.start()
            loads.append(copy)

    barrier = pltpu.get_barrier_semaphore()
    for dz, k in NEAR:
        pl.semaphore_signal(
            barrier, inc=1, device_id=at(peer_of(me, dz, k)), device_id_type=pl.DeviceIdType.MESH
        )
    for d in range(1, COLUMNS):
        pl.semaphore_signal(
            barrier, inc=1, device_id=(me, (col + d) % COLUMNS), device_id_type=pl.DeviceIdType.MESH
        )

    load_weight = pltpu.make_async_copy(weight_ref, weight, w_sem)
    load_weight.start()

    mine = pl.multiple_of(me * PIECE, PIECE)

    def send_row(m, dz, k):
        peer = peer_of(me, dz, k)
        pltpu.make_async_remote_copy(
            src_ref=moved_ref.at[peer, m],
            dst_ref=land.at[m, pl.ds(mine, PIECE), :],
            send_sem=f_send.at[m],
            recv_sem=f_recv.at[m],
            device_id=at(peer),
            device_id_type=pl.DeviceIdType.MESH,
        ).start()

    def send_rows(m, dz, low):
        def one(k, _):
            send_row(m, dz, k)
            return 0

        lax.fori_loop(low, 8, one, 0)

    for i, dz in enumerate(DZ_ORDER):
        block = pl.ds(((z + dz) % 8) * 8, 8)
        loads[2 * i].wait()
        loads[2 * i + 1].wait()
        moved_ref[block] = hold_rate * mom[block] + grad[block]
        if i == 0:
            pl.semaphore_wait(barrier, len(NEAR) + COLUMNS - 1)
            for far in DZ_ORDER[:-1]:
                pl.semaphore_signal(
                    ready, inc=1, device_id=at(peer_of(me, far, 0)), device_id_type=pl.DeviceIdType.MESH
                )
        if dz:
            for m in range(EARLY):
                for k in (0, 1):
                    send_row(m, dz, k)

    pl.semaphore_wait(ready, len(DZ_ORDER) - 1)
    for m in range(OWNED):
        for dz in DZ_ORDER:
            send_rows(m, dz, 1 if dz == 0 else 2 if m < EARLY else 0)
    for m in range(OWNED):
        land[m, pl.ds(mine, PIECE), :] = moved_ref[me, m]

    def tile_pair(m, j):
        sides = []
        for q in (2 * j, 2 * j + 1):
            sides.append(
                jnp.concatenate(
                    [land[m, pl.ds(2 * q + r, GROUPS, stride=PIECE), :] for r in (0, 1)], axis=0
                )
            )
        return jnp.concatenate(sides, axis=1)

    def wait_bytes(ref, sem):
        pltpu.make_async_copy(ref, ref, sem).wait()

    rows = lax.broadcasted_iota(jnp.int32, (SIDE, SIDE), 0)
    cols = lax.broadcasted_iota(jnp.int32, (SIDE, SIDE), 1)
    eye = jnp.where(rows == cols, 1.0, 0.0).astype(jnp.float32)

    def gram(m):
        wait_bytes(land.at[m, pl.ds(0, (GROUPS - 1) * PIECE), :], f_recv.at[m])
        total = None
        for j in range(TILES // 2):
            x = tile_pair(m, j)
            term = dot(x, x, 1, 1)
            total = term if total is None else total + term
        parts[m, col] = total
        for d in range(1, COLUMNS):
            pltpu.make_async_remote_copy(
                src_ref=parts.at[m, col],
                dst_ref=parts.at[m, col],
                send_sem=g_send.at[m],
                recv_sem=g_recv.at[m],
                device_id=(me, (col + d) % COLUMNS),
                device_id_type=pl.DeviceIdType.MESH,
            ).start()

    def finish(m):
        wait_bytes(parts.at[m, pl.ds(0, COLUMNS - 1)], g_recv.at[m])
        whole = (parts[m, 0] + parts[m, 1]) + (parts[m, 2] + parts[m, 3])
        power = jnp.sum(jnp.sum(whole * eye, axis=1, keepdims=True), axis=0, keepdims=True)
        scale = lax.rsqrt(power + 1e-06)
        a = whole * (scale * scale)
        product = None
        for step in range(ITERS):
            mixed = 3.4445 * eye - 4.775 * a + 2.0315 * dot(a, a, 1, 0)
            product = mixed if product is None else dot(mixed, product, 1, 0)
            if step < ITERS - 1:
                a = dot(dot(mixed, a, 1, 0), mixed, 1, 0)
        product = product * scale
        for j in range(TILES // 2):
            y = dot(product, tile_pair(m, j), 1, 0)
            for i in (0, 1):
                q = 2 * j + i
                for r in (0, 1):
                    res[m, pl.ds(2 * q + r, GROUPS, stride=PIECE), :] = y[
                        GROUPS * r : GROUPS * (r + 1), LANES * i : LANES * (i + 1)
                    ]
        for dz in DZ_ORDER:
            def one(k, _, dz=dz):
                peer = peer_of(me, dz, k)
                pltpu.make_async_remote_copy(
                    src_ref=res.at[m, pl.ds(pl.multiple_of(peer * PIECE, PIECE), PIECE), :],
                    dst_ref=back.at[me, m],
                    send_sem=b_send.at[m],
                    recv_sem=b_recv.at[m],
                    device_id=at(peer),
                    device_id_type=pl.DeviceIdType.MESH,
                ).start()
                return 0
            lax.fori_loop(1 if dz == 0 else 0, 8, one, 0)
        back[me, m] = res[m, pl.ds(mine, PIECE), :]

    gram(0)
    for m in range(OWNED):
        if m + 1 < OWNED:
            pass
        finish(m)
        if m + 1 < OWNED:
            gram(m + 1)

    load_weight.wait()
    for m in range(OWNED):
        wait_bytes(back.at[pl.ds(0, GROUPS - 1), m], b_recv.at[m])
        new_weight_ref[:, m] = weight[:, m] - learn_rate * back[:, m]

    for m in range(OWNED):
        wait_bytes(land.at[m, pl.ds(0, (GROUPS - 1) * PIECE), :], f_send.at[m])
        wait_bytes(parts.at[m, pl.ds(0, COLUMNS - 1)], g_send.at[m])
        wait_bytes(res.at[m, pl.ds(0, (GROUPS - 1) * PIECE), :], b_send.at[m])


def update(gradients, momentum, weights):
    whole = pltpu.VMEM(gradients.shape, jnp.float32)
    return pl.pallas_call(
        kernel,
        out_shape=[jax.ShapeDtypeStruct(gradients.shape, jnp.float32)] * 2,
        in_specs=[pl.BlockSpec(memory_space=pltpu.HBM)] * 3,
        out_specs=[pl.BlockSpec(memory_space=pltpu.VMEM)] * 2,
        scratch_shapes=[
            whole,
            whole,
            whole,
            pltpu.VMEM((OWNED, GROUPS * PIECE, LANES), jnp.float32),
            pltpu.VMEM((OWNED, GROUPS * PIECE, LANES), jnp.float32),
            pltpu.VMEM((OWNED, COLUMNS, SIDE, SIDE), jnp.float32),
            whole,
            pltpu.SemaphoreType.REGULAR,
            pltpu.SemaphoreType.DMA((16,)),
            pltpu.SemaphoreType.DMA,
            pltpu.SemaphoreType.DMA((OWNED,)),
            pltpu.SemaphoreType.DMA((OWNED,)),
            pltpu.SemaphoreType.DMA((OWNED,)),
            pltpu.SemaphoreType.DMA((OWNED,)),
            pltpu.SemaphoreType.DMA((OWNED,)),
            pltpu.SemaphoreType.DMA((OWNED,)),
        ],
        compiler_params=pltpu.CompilerParams(
            collective_id=0, has_side_effects=True, vmem_limit_bytes=48 * 1024 * 1024
        ),
    )(gradients, momentum, weights)


def store_kernel(new_weight_ref, moved_ref, weight_out, moved_out, sems):
    copies = [
        pltpu.make_async_copy(new_weight_ref, weight_out, sems.at[0]),
        pltpu.make_async_copy(moved_ref, moved_out, sems.at[1]),
    ]
    for copy in copies:
        copy.start()
    for copy in copies:
        copy.wait()


def store(new_weights, new_momentum):
    return pl.pallas_call(
        store_kernel,
        out_shape=[jax.ShapeDtypeStruct(new_weights.shape, jnp.float32)] * 2,
        in_specs=[pl.BlockSpec(memory_space=pltpu.VMEM)] * 2,
        out_specs=[pl.BlockSpec(memory_space=pltpu.HBM)] * 2,
        scratch_shapes=[pltpu.SemaphoreType.DMA((2,))],
        compiler_params=pltpu.CompilerParams(vmem_limit_bytes=1024 * 1024),
    )(new_weights, new_momentum)


def to_pieces(block):
    block = block.reshape(GROUPS, OWNED, 2, TILES, LANES).transpose(0, 1, 3, 2, 4)
    return block.reshape(GROUPS, OWNED, PIECE, LANES)


def from_pieces(pieces):
    pieces = pieces.reshape(GROUPS, OWNED, TILES, 2, LANES).transpose(0, 1, 3, 2, 4)
    return pieces.reshape(GROUPS * OWNED, 2, TILES * LANES)


def on_device(gradients, momentum, weights):
    new_weights, new_momentum = store(
        *update(to_pieces(gradients), to_pieces(momentum), to_pieces(weights))
    )
    return (from_pieces(new_weights), from_pieces(new_momentum))


def solution(mesh):
    placed = (P(None, "shard", "model"), P(None, "shard", "model"), P(None, "shard", "model"))
    return jax.shard_map(
        on_device,
        mesh=mesh,
        in_specs=placed,
        out_specs=(P(None, "shard", "model"), P(None, "shard", "model")),
        check_vma=False,
    )
```

```python
import functools

import jax
import jax.numpy as jnp
from jax import lax
from jax.experimental import pallas as pl
from jax.experimental.pallas import tpu as pltpu
from jax.sharding import PartitionSpec as P

ITERS = 4
hold_rate = 0.8
learn_rate = 1.0

GROUPS = 64
COLUMNS = 4
OWNED = 4
SIDE = 128
LANES = 128
TILES = 8
PIECE = 16
DZ_ORDER = (4, 3, 5, 2, 6, 1, 7, 0)
NEAR = [(dz, k) for dz in DZ_ORDER[:-1] for k in (0, 1)] + [(0, k) for k in (4, 5, 2, 3, 6, 7, 1)]
EARLY = 2
BY_DISTANCE = 3
Z_ORDER = ((0,), (1, 2), (3, 7), (4, 5, 6))
HIGH = lax.Precision.HIGHEST


def dot(a, b, ca, cb):
    return lax.dot_general(
        a, b, (((ca,), (cb,)), ((), ())), precision=HIGH, preferred_element_type=jnp.float32
    )


def peer_of(me, dz, k):
    z, y, core = me // 8, (me // 2) % 4, me % 2
    return ((z + dz) % 8) * 8 + ((y + k // 2) % 4) * 2 + (core + k % 2) % 2


def kernel(
    grad_ref, mom_ref, weight_ref, new_weight_ref, moved_ref,
    grad, mom, weight, land, res, parts, back,
    ready, in_sem, w_sem, f_send, f_recv, g_send, g_recv, b_send, b_recv,
):
    me = lax.axis_index("shard")
    col = lax.axis_index("model")

    def at(peer):
        return (peer, col)

    z = me // 8
    loads = []
    for i, dz in enumerate(DZ_ORDER):
        block = pl.ds(((z + dz) % 8) * 8, 8)
        for j, (ref, buf) in enumerate(((grad_ref, grad), (mom_ref, mom))):
            copy = pltpu.make_async_copy(ref.at[block], buf.at[block], in_sem.at[2 * i + j])
            copy.start()
            loads.append(copy)

    barrier = pltpu.get_barrier_semaphore()
    for dz, k in NEAR:
        pl.semaphore_signal(
            barrier, inc=1, device_id=at(peer_of(me, dz, k)), device_id_type=pl.DeviceIdType.MESH
        )
    for d in range(1, COLUMNS):
        pl.semaphore_signal(
            barrier, inc=1, device_id=(me, (col + d) % COLUMNS), device_id_type=pl.DeviceIdType.MESH
        )

    load_weight = pltpu.make_async_copy(weight_ref, weight, w_sem)
    load_weight.start()

    mine = pl.multiple_of(me * PIECE, PIECE)

    def send_row(m, dz, k):
        peer = peer_of(me, dz, k)
        pltpu.make_async_remote_copy(
            src_ref=moved_ref.at[peer, m],
            dst_ref=land.at[m, pl.ds(mine, PIECE), :],
            send_sem=f_send.at[m],
            recv_sem=f_recv.at[m],
            device_id=at(peer),
            device_id_type=pl.DeviceIdType.MESH,
        ).start()

    def send_rows(m, dz, low):
        def one(k, _):
            send_row(m, dz, k)
            return 0

        lax.fori_loop(low, 8, one, 0)

    for i, dz in enumerate(DZ_ORDER):
        block = pl.ds(((z + dz) % 8) * 8, 8)
        loads[2 * i].wait()
        loads[2 * i + 1].wait()
        moved_ref[block] = hold_rate * mom[block] + grad[block]
        if i == 0:
            pl.semaphore_wait(barrier, len(NEAR) + COLUMNS - 1)
            for far in DZ_ORDER[:-1]:
                pl.semaphore_signal(
                    ready, inc=1, device_id=at(peer_of(me, far, 0)), device_id_type=pl.DeviceIdType.MESH
                )
        if dz:
            for m in range(EARLY):
                for k in (0, 1):
                    send_row(m, dz, k)

    pl.semaphore_wait(ready, len(DZ_ORDER) - 1)
    for m in range(OWNED):
        for dz in DZ_ORDER:
            send_rows(m, dz, 1 if dz == 0 else 2 if m < EARLY else 0)
    for m in range(OWNED):
        land[m, pl.ds(mine, PIECE), :] = moved_ref[me, m]

    def tile_pair(m, j):
        sides = []
        for q in (2 * j, 2 * j + 1):
            sides.append(
                jnp.concatenate(
                    [land[m, pl.ds(2 * q + r, GROUPS, stride=PIECE), :] for r in (0, 1)], axis=0
                )
            )
        return jnp.concatenate(sides, axis=1)

    def wait_bytes(ref, sem):
        pltpu.make_async_copy(ref, ref, sem).wait()

    rows = lax.broadcasted_iota(jnp.int32, (SIDE, SIDE), 0)
    cols = lax.broadcasted_iota(jnp.int32, (SIDE, SIDE), 1)
    eye = jnp.where(rows == cols, 1.0, 0.0).astype(jnp.float32)

    def gram(m):
        wait_bytes(land.at[m, pl.ds(0, (GROUPS - 1) * PIECE), :], f_recv.at[m])
        total = None
        for j in range(TILES // 2):
            x = tile_pair(m, j)
            term = dot(x, x, 1, 1)
            total = term if total is None else total + term
        parts[m, col] = total
        for d in range(1, COLUMNS):
            pltpu.make_async_remote_copy(
                src_ref=parts.at[m, col],
                dst_ref=parts.at[m, col],
                send_sem=g_send.at[m],
                recv_sem=g_recv.at[m],
                device_id=(me, (col + d) % COLUMNS),
                device_id_type=pl.DeviceIdType.MESH,
            ).start()

    def finish(m):
        wait_bytes(parts.at[m, pl.ds(0, COLUMNS - 1)], g_recv.at[m])
        whole = (parts[m, 0] + parts[m, 1]) + (parts[m, 2] + parts[m, 3])
        power = jnp.sum(jnp.sum(whole * eye, axis=1, keepdims=True), axis=0, keepdims=True)
        scale = lax.rsqrt(power + 1e-06)
        a = whole * (scale * scale)
        product = None
        for step in range(ITERS):
            mixed = 3.4445 * eye - 4.775 * a + 2.0315 * dot(a, a, 1, 0)
            product = mixed if product is None else dot(mixed, product, 1, 0)
            if step < ITERS - 1:
                a = dot(dot(mixed, a, 1, 0), mixed, 1, 0)
        product = product * scale
        for j in range(TILES // 2):
            y = dot(product, tile_pair(m, j), 1, 0)
            for i in (0, 1):
                q = 2 * j + i
                for r in (0, 1):
                    res[m, pl.ds(2 * q + r, GROUPS, stride=PIECE), :] = y[
                        GROUPS * r : GROUPS * (r + 1), LANES * i : LANES * (i + 1)
                    ]
        def send_back(peer):
            pltpu.make_async_remote_copy(
                src_ref=res.at[m, pl.ds(pl.multiple_of(peer * PIECE, PIECE), PIECE), :],
                dst_ref=back.at[me, m],
                send_sem=b_send.at[m],
                recv_sem=b_recv.at[m],
                device_id=at(peer),
                device_id_type=pl.DeviceIdType.MESH,
            ).start()

        if m < BY_DISTANCE:
            for dz in DZ_ORDER:
                def one(k, _, dz=dz):
                    send_back(peer_of(me, dz, k))
                    return 0

                lax.fori_loop(1 if dz == 0 else 0, 8, one, 0)
        else:
            for heres in Z_ORDER:
                def one(k, _, heres=heres):
                    for there in heres:
                        peer = there * 8 + k

                        @pl.when(peer != me)
                        def _():
                            send_back(peer)

                    return 0

                lax.fori_loop(0, 8, one, 0)
        back[me, m] = res[m, pl.ds(mine, PIECE), :]

    gram(0)
    for m in range(OWNED):
        if m + 1 < OWNED:
            pass
        finish(m)
        if m + 1 < OWNED:
            gram(m + 1)

    load_weight.wait()
    for m in range(OWNED):
        wait_bytes(back.at[pl.ds(0, GROUPS - 1), m], b_recv.at[m])
        new_weight_ref[:, m] = weight[:, m] - learn_rate * back[:, m]

    for m in range(OWNED):
        wait_bytes(land.at[m, pl.ds(0, (GROUPS - 1) * PIECE), :], f_send.at[m])
        wait_bytes(parts.at[m, pl.ds(0, COLUMNS - 1)], g_send.at[m])
        wait_bytes(res.at[m, pl.ds(0, (GROUPS - 1) * PIECE), :], b_send.at[m])


def update(gradients, momentum, weights):
    whole = pltpu.VMEM(gradients.shape, jnp.float32)
    return pl.pallas_call(
        kernel,
        out_shape=[jax.ShapeDtypeStruct(gradients.shape, jnp.float32)] * 2,
        in_specs=[pl.BlockSpec(memory_space=pltpu.HBM)] * 3,
        out_specs=[pl.BlockSpec(memory_space=pltpu.VMEM)] * 2,
        scratch_shapes=[
            whole,
            whole,
            whole,
            pltpu.VMEM((OWNED, GROUPS * PIECE, LANES), jnp.float32),
            pltpu.VMEM((OWNED, GROUPS * PIECE, LANES), jnp.float32),
            pltpu.VMEM((OWNED, COLUMNS, SIDE, SIDE), jnp.float32),
            whole,
            pltpu.SemaphoreType.REGULAR,
            pltpu.SemaphoreType.DMA((16,)),
            pltpu.SemaphoreType.DMA,
            pltpu.SemaphoreType.DMA((OWNED,)),
            pltpu.SemaphoreType.DMA((OWNED,)),
            pltpu.SemaphoreType.DMA((OWNED,)),
            pltpu.SemaphoreType.DMA((OWNED,)),
            pltpu.SemaphoreType.DMA((OWNED,)),
            pltpu.SemaphoreType.DMA((OWNED,)),
        ],
        compiler_params=pltpu.CompilerParams(
            collective_id=0, has_side_effects=True, vmem_limit_bytes=48 * 1024 * 1024
        ),
    )(gradients, momentum, weights)


def store_kernel(new_weight_ref, moved_ref, weight_out, moved_out, sems):
    copies = [
        pltpu.make_async_copy(new_weight_ref, weight_out, sems.at[0]),
        pltpu.make_async_copy(moved_ref, moved_out, sems.at[1]),
    ]
    for copy in copies:
        copy.start()
    for copy in copies:
        copy.wait()


def store(new_weights, new_momentum):
    return pl.pallas_call(
        store_kernel,
        out_shape=[jax.ShapeDtypeStruct(new_weights.shape, jnp.float32)] * 2,
        in_specs=[pl.BlockSpec(memory_space=pltpu.VMEM)] * 2,
        out_specs=[pl.BlockSpec(memory_space=pltpu.HBM)] * 2,
        scratch_shapes=[pltpu.SemaphoreType.DMA((2,))],
        compiler_params=pltpu.CompilerParams(vmem_limit_bytes=1024 * 1024),
    )(new_weights, new_momentum)


def to_pieces(block):
    block = block.reshape(GROUPS, OWNED, 2, TILES, LANES).transpose(0, 1, 3, 2, 4)
    return block.reshape(GROUPS, OWNED, PIECE, LANES)


def from_pieces(pieces):
    pieces = pieces.reshape(GROUPS, OWNED, TILES, 2, LANES).transpose(0, 1, 3, 2, 4)
    return pieces.reshape(GROUPS * OWNED, 2, TILES * LANES)


def on_device(gradients, momentum, weights):
    new_weights, new_momentum = store(
        *update(to_pieces(gradients), to_pieces(momentum), to_pieces(weights))
    )
    return (from_pieces(new_weights), from_pieces(new_momentum))


def solution(mesh):
    placed = (P(None, "shard", "model"), P(None, "shard", "model"), P(None, "shard", "model"))
    return jax.shard_map(
        on_device,
        mesh=mesh,
        in_specs=placed,
        out_specs=(P(None, "shard", "model"), P(None, "shard", "model")),
        check_vma=False,
    )
```

```python
import functools

import jax
import jax.numpy as jnp
from jax import lax
from jax.experimental import pallas as pl
from jax.experimental.pallas import tpu as pltpu
from jax.sharding import PartitionSpec as P

ITERS = 4
hold_rate = 0.8
learn_rate = 1.0

GROUPS = 64
COLUMNS = 4
OWNED = 4
SIDE = 128
LANES = 128
TILES = 8
PIECE = 16
DZ_ORDER = (4, 3, 5, 2, 6, 1, 7, 0)
FIRST = (0, 1)
NEAR = [(dz, k) for dz in (1, 7) for k in FIRST] + [(0, k) for k in (4, 5, 2, 3, 6, 7, 1)]
LOAD_ORDER = (1, 7, 2, 6, 3, 5, 4, 0)
W2 = 1
W3 = 1
BY_DISTANCE = 3
Z_LATE = (0.0, 0.9, 1.9, 2.8, 3.9, 4.8, 4.8, 3.9)
Y_LATE = (0.0, 0.8, 1.6, 1.8)
CELLS = sorted(range(32), key=lambda cell: (1 * Z_LATE[cell // 4] + 2 * Y_LATE[cell % 4], cell))
HIGH = lax.Precision.HIGHEST


def dot(a, b, ca, cb):
    return lax.dot_general(
        a, b, (((ca,), (cb,)), ((), ())), precision=HIGH, preferred_element_type=jnp.float32
    )


def peer_of(me, dz, k):
    z, y, core = me // 8, (me // 2) % 4, me % 2
    return ((z + dz) % 8) * 8 + ((y + k // 2) % 4) * 2 + (core + k % 2) % 2


def kernel(
    grad_ref, mom_ref, weight_ref, new_weight_ref, moved_ref,
    grad, mom, weight, land, res, parts, back, mid,
    ready, in_sem, w_sem, f_send, f_recv, g_send, g_recv, b_send, b_recv,
):
    me = lax.axis_index("shard")
    col = lax.axis_index("model")

    def at(peer):
        return (peer, col)

    z = me // 8
    loads = []

    def load(i, dz):
        block = pl.ds(((z + dz) % 8) * 8, 8)
        for j, (ref, buf) in enumerate(((grad_ref, grad), (mom_ref, mom))):
            copy = pltpu.make_async_copy(ref.at[block], buf.at[block], in_sem.at[2 * i + j])
            copy.start()
            loads.append(copy)

    def signal(sem, dz, k):
        pl.semaphore_signal(
            sem, inc=1, device_id=at(peer_of(me, dz, k)), device_id_type=pl.DeviceIdType.MESH
        )

    load(0, LOAD_ORDER[0])
    barrier = pltpu.get_barrier_semaphore()
    for dz, k in NEAR:
        signal(barrier, dz, k)
    for d in range(1, COLUMNS):
        pl.semaphore_signal(
            barrier, inc=1, device_id=(me, (col + d) % COLUMNS), device_id_type=pl.DeviceIdType.MESH
        )
    for i, dz in enumerate(LOAD_ORDER):
        if i:
            load(i, dz)
    load_weight = pltpu.make_async_copy(weight_ref, weight, w_sem)
    load_weight.start()

    mine = pl.multiple_of(me * PIECE, PIECE)

    def momentum_of(i):
        block = pl.ds(((z + LOAD_ORDER[i]) % 8) * 8, 8)
        loads[2 * i].wait()
        loads[2 * i + 1].wait()
        moved_ref[block] = hold_rate * mom[block] + grad[block]

    def send_row(m, dz, k):
        peer = peer_of(me, dz, k)
        pltpu.make_async_remote_copy(
            src_ref=moved_ref.at[peer, m],
            dst_ref=land.at[m, pl.ds(mine, PIECE), :],
            send_sem=f_send.at[m],
            recv_sem=f_recv.at[m],
            device_id=at(peer),
            device_id_type=pl.DeviceIdType.MESH,
        ).start()

    def send_rows(m, dz, low):
        def one(k, _):
            send_row(m, dz, k)
            return 0

        lax.fori_loop(low, 8, one, 0)

    def meet(round_):
        for dz in (1, 7):
            signal(ready.at[round_], dz, 0)

    def met(round_):
        pl.semaphore_wait(ready.at[round_], 2)

    momentum_of(0)
    momentum_of(1)
    pl.semaphore_wait(barrier, len(NEAR) + COLUMNS - 1)
    meet(0)
    for m in range(OWNED):
        for dz in (1, 7):
            for k in FIRST:
                send_row(m, dz, k)
    for i in range(2, 8):
        momentum_of(i)
    met(0)
    meet(1)
    for m in range(OWNED):
        for dz in (1, 7):
            send_rows(m, dz, len(FIRST))
    met(1)
    meet(2)
    for m in range(W2):
        for dz in (2, 6):
            send_rows(m, dz, 0)
    met(2)
    meet(3)
    for m in range(W3):
        for dz in (3, 5):
            send_rows(m, dz, 0)
    met(3)
    for m in range(OWNED):
        for dz in (4, 3, 5, 2, 6, 0):
            if (dz in (3, 5) and m < W3) or (dz in (2, 6) and m < W2):
                continue
            send_rows(m, dz, 1 if dz == 0 else 0)
    for m in range(OWNED):
        land[m, pl.ds(mine, PIECE), :] = moved_ref[me, m]

    def tile_pair(m, j):
        sides = []
        for q in (2 * j, 2 * j + 1):
            sides.append(
                jnp.concatenate(
                    [land[m, pl.ds(2 * q + r, GROUPS, stride=PIECE), :] for r in (0, 1)], axis=0
                )
            )
        return jnp.concatenate(sides, axis=1)

    def wait_bytes(ref, sem):
        pltpu.make_async_copy(ref, ref, sem).wait()

    rows = lax.broadcasted_iota(jnp.int32, (SIDE, SIDE), 0)
    cols = lax.broadcasted_iota(jnp.int32, (SIDE, SIDE), 1)
    eye = jnp.where(rows == cols, 1.0, 0.0).astype(jnp.float32)

    def gram(m):
        wait_bytes(land.at[m, pl.ds(0, (GROUPS - 1) * PIECE), :], f_recv.at[m])
        total = None
        for j in range(TILES // 2):
            x = tile_pair(m, j)
            term = dot(x, x, 1, 1)
            total = term if total is None else total + term
        parts[m, col] = total
        for d in range(1, COLUMNS):
            pltpu.make_async_remote_copy(
                src_ref=parts.at[m, col],
                dst_ref=parts.at[m, col],
                send_sem=g_send.at[m],
                recv_sem=g_recv.at[m],
                device_id=(me, (col + d) % COLUMNS),
                device_id_type=pl.DeviceIdType.MESH,
            ).start()

    def finish(m):
        wait_bytes(parts.at[m, pl.ds(0, COLUMNS - 1)], g_recv.at[m])
        whole = (parts[m, 0] + parts[m, 1]) + (parts[m, 2] + parts[m, 3])
        power = jnp.sum(jnp.sum(whole * eye, axis=1, keepdims=True), axis=0, keepdims=True)
        scale = lax.rsqrt(power + 1e-06)
        a = whole * (scale * scale)
        for step in range(ITERS):
            rest = -4.775 * a + 2.0315 * dot(a, a, 1, 0)
            if step < ITERS - 1:
                mixed = 3.4445 * eye + rest
                a = dot(dot(mixed, a, 1, 0), mixed, 1, 0)
            for j in range(TILES // 2):
                x = tile_pair(m, j) * scale if step == 0 else mid[j]
                y = 3.4445 * x + dot(rest, x, 1, 0)
                if step < ITERS - 1:
                    mid[j] = y
                else:
                    for i in (0, 1):
                        q = 2 * j + i
                        for r in (0, 1):
                            res[m, pl.ds(2 * q + r, GROUPS, stride=PIECE), :] = y[
                                GROUPS * r : GROUPS * (r + 1), LANES * i : LANES * (i + 1)
                            ]

        def send_back(peer):
            pltpu.make_async_remote_copy(
                src_ref=res.at[m, pl.ds(pl.multiple_of(peer * PIECE, PIECE), PIECE), :],
                dst_ref=back.at[me, m],
                send_sem=b_send.at[m],
                recv_sem=b_recv.at[m],
                device_id=at(peer),
                device_id_type=pl.DeviceIdType.MESH,
            ).start()

        if m < BY_DISTANCE:
            for dz in DZ_ORDER:
                def one(k, _, dz=dz):
                    send_back(peer_of(me, dz, k))
                    return 0

                lax.fori_loop(1 if dz == 0 else 0, 8, one, 0)
        else:
            for cell in CELLS:
                for peer in (2 * cell + 1, 2 * cell):

                    @pl.when(peer != me)
                    def _(peer=peer):
                        send_back(peer)

        back[me, m] = res[m, pl.ds(mine, PIECE), :]

    gram(0)
    for m in range(OWNED):
        if m + 1 < OWNED:
            pass
        finish(m)
        if m + 1 < OWNED:
            gram(m + 1)

    load_weight.wait()
    for m in range(OWNED):
        wait_bytes(back.at[pl.ds(0, GROUPS - 1), m], b_recv.at[m])
        new_weight_ref[:, m] = weight[:, m] - learn_rate * back[:, m]

    for m in range(OWNED):
        wait_bytes(land.at[m, pl.ds(0, (GROUPS - 1) * PIECE), :], f_send.at[m])
        wait_bytes(parts.at[m, pl.ds(0, COLUMNS - 1)], g_send.at[m])
        wait_bytes(res.at[m, pl.ds(0, (GROUPS - 1) * PIECE), :], b_send.at[m])


def update(gradients, momentum, weights):
    whole = pltpu.VMEM(gradients.shape, jnp.float32)
    return pl.pallas_call(
        kernel,
        out_shape=[jax.ShapeDtypeStruct(gradients.shape, jnp.float32)] * 2,
        in_specs=[pl.BlockSpec(memory_space=pltpu.HBM)] * 3,
        out_specs=[pl.BlockSpec(memory_space=pltpu.VMEM)] * 2,
        scratch_shapes=[
            whole,
            whole,
            whole,
            pltpu.VMEM((OWNED, GROUPS * PIECE, LANES), jnp.float32),
            pltpu.VMEM((OWNED, GROUPS * PIECE, LANES), jnp.float32),
            pltpu.VMEM((OWNED, COLUMNS, SIDE, SIDE), jnp.float32),
            whole,
            pltpu.VMEM((TILES // 2, SIDE, 2 * LANES), jnp.float32),
            pltpu.SemaphoreType.REGULAR((4,)),
            pltpu.SemaphoreType.DMA((16,)),
            pltpu.SemaphoreType.DMA,
            pltpu.SemaphoreType.DMA((OWNED,)),
            pltpu.SemaphoreType.DMA((OWNED,)),
            pltpu.SemaphoreType.DMA((OWNED,)),
            pltpu.SemaphoreType.DMA((OWNED,)),
            pltpu.SemaphoreType.DMA((OWNED,)),
            pltpu.SemaphoreType.DMA((OWNED,)),
        ],
        compiler_params=pltpu.CompilerParams(
            collective_id=0, has_side_effects=True, vmem_limit_bytes=48 * 1024 * 1024
        ),
    )(gradients, momentum, weights)


def store_kernel(new_weight_ref, moved_ref, weight_out, moved_out, sems):
    copies = [
        pltpu.make_async_copy(new_weight_ref, weight_out, sems.at[0]),
        pltpu.make_async_copy(moved_ref, moved_out, sems.at[1]),
    ]
    for copy in copies:
        copy.start()
    for copy in copies:
        copy.wait()


def store(new_weights, new_momentum):
    return pl.pallas_call(
        store_kernel,
        out_shape=[jax.ShapeDtypeStruct(new_weights.shape, jnp.float32)] * 2,
        in_specs=[pl.BlockSpec(memory_space=pltpu.VMEM)] * 2,
        out_specs=[pl.BlockSpec(memory_space=pltpu.HBM)] * 2,
        scratch_shapes=[pltpu.SemaphoreType.DMA((2,))],
        compiler_params=pltpu.CompilerParams(vmem_limit_bytes=1024 * 1024),
    )(new_weights, new_momentum)


def to_pieces(block):
    block = block.reshape(GROUPS, OWNED, 2, TILES, LANES).transpose(0, 1, 3, 2, 4)
    return block.reshape(GROUPS, OWNED, PIECE, LANES)


def from_pieces(pieces):
    pieces = pieces.reshape(GROUPS, OWNED, TILES, 2, LANES).transpose(0, 1, 3, 2, 4)
    return pieces.reshape(GROUPS * OWNED, 2, TILES * LANES)


def on_device(gradients, momentum, weights):
    new_weights, new_momentum = store(
        *update(to_pieces(gradients), to_pieces(momentum), to_pieces(weights))
    )
    return (from_pieces(new_weights), from_pieces(new_momentum))


def solution(mesh):
    placed = (P(None, "shard", "model"), P(None, "shard", "model"), P(None, "shard", "model"))
    return jax.shard_map(
        on_device,
        mesh=mesh,
        in_specs=placed,
        out_specs=(P(None, "shard", "model"), P(None, "shard", "model")),
        check_vma=False,
    )
```

```python
import functools

import jax
import jax.numpy as jnp
from jax import lax
from jax.experimental import pallas as pl
from jax.experimental.pallas import tpu as pltpu
from jax.sharding import PartitionSpec as P

ITERS = 4
hold_rate = 0.8
learn_rate = 1.0

GROUPS = 64
COLUMNS = 4
OWNED = 4
SIDE = 128
LANES = 128
TILES = 8
PIECE = 16
DZ_ORDER = (4, 3, 5, 2, 6, 1, 7, 0)
FIRST = (0, 1)
NEAR = [(dz, k) for dz in (1, 7) for k in FIRST] + [(0, k) for k in (4, 5, 2, 3, 6, 7, 1)]
LOAD_ORDER = (1, 7, 2, 6, 3, 5, 4, 0)
W2 = 1
W3 = 1
BY_DISTANCE = 3
Z_LATE = (0.0, 0.9, 1.9, 2.8, 3.9, 4.8, 4.8, 3.9)
Y_LATE = (0.0, 0.8, 1.6, 1.8)
CELLS = sorted(range(32), key=lambda cell: (1 * Z_LATE[cell // 4] + 2 * Y_LATE[cell % 4], cell))
HIGH = lax.Precision.HIGHEST


def dot(a, b, ca, cb):
    return lax.dot_general(
        a, b, (((ca,), (cb,)), ((), ())), precision=HIGH, preferred_element_type=jnp.float32
    )


def peer_of(me, dz, k):
    z, y, core = me // 8, (me // 2) % 4, me % 2
    return ((z + dz) % 8) * 8 + ((y + k // 2) % 4) * 2 + (core + k % 2) % 2


def kernel(
    grad_ref, mom_ref, weight_ref, new_weight_ref, moved_ref,
    grad, mom, weight, land, res, parts, back, mid,
    ready, in_sem, w_sem, f_send, f_recv, g_send, g_recv, b_send, b_recv,
):
    me = lax.axis_index("shard")
    col = lax.axis_index("model")

    def at(peer):
        return (peer, col)

    z = me // 8
    loads = []

    def load(i, dz):
        block = pl.ds(((z + dz) % 8) * 8, 8)
        for j, (ref, buf) in enumerate(((grad_ref, grad), (mom_ref, mom))):
            copy = pltpu.make_async_copy(ref.at[block], buf.at[block], in_sem.at[2 * i + j])
            copy.start()
            loads.append(copy)

    def signal(sem, dz, k):
        pl.semaphore_signal(
            sem, inc=1, device_id=at(peer_of(me, dz, k)), device_id_type=pl.DeviceIdType.MESH
        )

    load(0, LOAD_ORDER[0])
    barrier = pltpu.get_barrier_semaphore()
    for dz, k in NEAR:
        signal(barrier, dz, k)
    for d in range(1, COLUMNS):
        pl.semaphore_signal(
            barrier, inc=1, device_id=(me, (col + d) % COLUMNS), device_id_type=pl.DeviceIdType.MESH
        )
    for i, dz in enumerate(LOAD_ORDER):
        if i:
            load(i, dz)
    load_weight = pltpu.make_async_copy(weight_ref, weight, w_sem)
    load_weight.start()

    mine = pl.multiple_of(me * PIECE, PIECE)

    def momentum_of(i):
        block = pl.ds(((z + LOAD_ORDER[i]) % 8) * 8, 8)
        loads[2 * i].wait()
        loads[2 * i + 1].wait()
        moved_ref[block] = hold_rate * mom[block] + grad[block]

    def send_row(m, dz, k):
        peer = peer_of(me, dz, k)
        pltpu.make_async_remote_copy(
            src_ref=moved_ref.at[peer, m],
            dst_ref=land.at[m, pl.ds(mine, PIECE), :],
            send_sem=f_send.at[m],
            recv_sem=f_recv.at[m],
            device_id=at(peer),
            device_id_type=pl.DeviceIdType.MESH,
        ).start()

    def send_rows(m, dz, low):
        def one(k, _):
            send_row(m, dz, k)
            return 0

        lax.fori_loop(low, 8, one, 0)

    def meet(round_):
        for dz in (1, 7):
            signal(ready.at[round_], dz, 0)

    def met(round_):
        pl.semaphore_wait(ready.at[round_], 2)

    momentum_of(0)
    momentum_of(1)
    pl.semaphore_wait(barrier, len(NEAR) + COLUMNS - 1)
    meet(0)
    for m in range(OWNED):
        for dz in (1, 7):
            for k in FIRST:
                send_row(m, dz, k)
    for i in range(2, 8):
        momentum_of(i)
    met(0)
    meet(1)
    for m in range(OWNED):
        for dz in (1, 7):
            send_rows(m, dz, len(FIRST))
    met(1)
    meet(2)
    for m in range(W2):
        for dz in (2, 6):
            send_rows(m, dz, 0)
    met(2)
    meet(3)
    for m in range(W3):
        for dz in (3, 5):
            send_rows(m, dz, 0)
    met(3)
    for m in range(OWNED):
        for dz in (4, 3, 5, 2, 6, 0):
            if (dz in (3, 5) and m < W3) or (dz in (2, 6) and m < W2):
                continue
            send_rows(m, dz, 1 if dz == 0 else 0)
    for m in range(OWNED):
        land[m, pl.ds(mine, PIECE), :] = moved_ref[me, m]

    def tile_pair(m, j):
        sides = []
        for q in (2 * j, 2 * j + 1):
            sides.append(
                jnp.concatenate(
                    [land[m, pl.ds(2 * q + r, GROUPS, stride=PIECE), :] for r in (0, 1)], axis=0
                )
            )
        return jnp.concatenate(sides, axis=1)

    def wait_bytes(ref, sem):
        pltpu.make_async_copy(ref, ref, sem).wait()

    rows = lax.broadcasted_iota(jnp.int32, (SIDE, SIDE), 0)
    cols = lax.broadcasted_iota(jnp.int32, (SIDE, SIDE), 1)
    eye = jnp.where(rows == cols, 1.0, 0.0).astype(jnp.float32)

    def gram(m):
        wait_bytes(land.at[m, pl.ds(0, (GROUPS - 1) * PIECE), :], f_recv.at[m])
        total = None
        for j in range(TILES // 2):
            x = tile_pair(m, j)
            term = dot(x, x, 1, 1)
            total = term if total is None else total + term
        parts[m, col] = total
        for d in range(1, COLUMNS):
            pltpu.make_async_remote_copy(
                src_ref=parts.at[m, col],
                dst_ref=parts.at[m, col],
                send_sem=g_send.at[m],
                recv_sem=g_recv.at[m],
                device_id=(me, (col + d) % COLUMNS),
                device_id_type=pl.DeviceIdType.MESH,
            ).start()

    def finish(m):
        wait_bytes(parts.at[m, pl.ds(0, COLUMNS - 1)], g_recv.at[m])
        whole = (parts[m, 0] + parts[m, 1]) + (parts[m, 2] + parts[m, 3])
        power = jnp.sum(jnp.sum(whole * eye, axis=1, keepdims=True), axis=0, keepdims=True)
        scale = lax.rsqrt(power + 1e-06)
        a = whole * (scale * scale)
        for step in range(ITERS):
            rest = -4.775 * a + 2.0315 * dot(a, a, 1, 0)
            if step < ITERS - 1:
                mixed = 3.4445 * eye + rest
                a = dot(dot(mixed, a, 1, 0), mixed, 1, 0)
            for j in range(TILES // 2):
                x = tile_pair(m, j) * scale if step == 0 else mid[j]
                y = 3.4445 * x + dot(rest, x, 1, 0)
                if step < ITERS - 1:
                    mid[j] = y
                else:
                    for i in (0, 1):
                        q = 2 * j + i
                        for r in (0, 1):
                            res[m, pl.ds(2 * q + r, GROUPS, stride=PIECE), :] = y[
                                GROUPS * r : GROUPS * (r + 1), LANES * i : LANES * (i + 1)
                            ]

        def send_back(peer):
            pltpu.make_async_remote_copy(
                src_ref=res.at[m, pl.ds(pl.multiple_of(peer * PIECE, PIECE), PIECE), :],
                dst_ref=back.at[me, m],
                send_sem=b_send.at[m],
                recv_sem=b_recv.at[m],
                device_id=at(peer),
                device_id_type=pl.DeviceIdType.MESH,
            ).start()

        if m < BY_DISTANCE:
            for dz in DZ_ORDER:
                def one(k, _, dz=dz):
                    send_back(peer_of(me, dz, k))
                    return 0

                lax.fori_loop(1 if dz == 0 else 0, 8, one, 0)
        else:
            for cell in CELLS:
                for peer in (2 * cell + 1, 2 * cell):

                    @pl.when(peer != me)
                    def _(peer=peer):
                        send_back(peer)

        back[me, m] = res[m, pl.ds(mine, PIECE), :]

    gram(0)
    for m in range(OWNED):
        if m + 1 < OWNED:
            pass
        finish(m)
        if m + 1 < OWNED:
            gram(m + 1)

    load_weight.wait()
    for m in range(OWNED):
        wait_bytes(back.at[pl.ds(0, GROUPS - 1), m], b_recv.at[m])
        new_weight_ref[:, m] = weight[:, m] - learn_rate * back[:, m]

    for m in range(OWNED):
        wait_bytes(land.at[m, pl.ds(0, (GROUPS - 1) * PIECE), :], f_send.at[m])
        wait_bytes(parts.at[m, pl.ds(0, COLUMNS - 1)], g_send.at[m])
        wait_bytes(res.at[m, pl.ds(0, (GROUPS - 1) * PIECE), :], b_send.at[m])


def update(gradients, momentum, weights):
    whole = pltpu.VMEM(gradients.shape, jnp.float32)
    return pl.pallas_call(
        kernel,
        out_shape=[jax.ShapeDtypeStruct(gradients.shape, jnp.float32)] * 2,
        in_specs=[pl.BlockSpec(memory_space=pltpu.HBM)] * 3,
        out_specs=[pl.BlockSpec(memory_space=pltpu.VMEM)] * 2,
        scratch_shapes=[
            whole,
            whole,
            whole,
            pltpu.VMEM((OWNED, GROUPS * PIECE, LANES), jnp.float32),
            pltpu.VMEM((OWNED, GROUPS * PIECE, LANES), jnp.float32),
            pltpu.VMEM((OWNED, COLUMNS, SIDE, SIDE), jnp.float32),
            whole,
            pltpu.VMEM((TILES // 2, SIDE, 2 * LANES), jnp.float32),
            pltpu.SemaphoreType.REGULAR((4,)),
            pltpu.SemaphoreType.DMA((16,)),
            pltpu.SemaphoreType.DMA,
            pltpu.SemaphoreType.DMA((OWNED,)),
            pltpu.SemaphoreType.DMA((OWNED,)),
            pltpu.SemaphoreType.DMA((OWNED,)),
            pltpu.SemaphoreType.DMA((OWNED,)),
            pltpu.SemaphoreType.DMA((OWNED,)),
            pltpu.SemaphoreType.DMA((OWNED,)),
        ],
        compiler_params=pltpu.CompilerParams(
            collective_id=0, has_side_effects=True, vmem_limit_bytes=48 * 1024 * 1024
        ),
    )(gradients, momentum, weights)


def store_kernel(new_weight_ref, moved_ref, weight_out, moved_out, sems):
    copies = [
        pltpu.make_async_copy(new_weight_ref, weight_out, sems.at[0]),
        pltpu.make_async_copy(moved_ref, moved_out, sems.at[1]),
    ]
    for i, copy in enumerate(copies):
        copy.start(priority=i)
    for copy in copies:
        copy.wait()


def store(new_weights, new_momentum):
    return pl.pallas_call(
        store_kernel,
        out_shape=[jax.ShapeDtypeStruct(new_weights.shape, jnp.float32)] * 2,
        in_specs=[pl.BlockSpec(memory_space=pltpu.VMEM)] * 2,
        out_specs=[pl.BlockSpec(memory_space=pltpu.HBM)] * 2,
        scratch_shapes=[pltpu.SemaphoreType.DMA((2,))],
        compiler_params=pltpu.CompilerParams(vmem_limit_bytes=1024 * 1024),
    )(new_weights, new_momentum)


def to_pieces(block):
    block = block.reshape(GROUPS, OWNED, 2, TILES, LANES).transpose(0, 1, 3, 2, 4)
    return block.reshape(GROUPS, OWNED, PIECE, LANES)


def from_pieces(pieces):
    pieces = pieces.reshape(GROUPS, OWNED, TILES, 2, LANES).transpose(0, 1, 3, 2, 4)
    return pieces.reshape(GROUPS * OWNED, 2, TILES * LANES)


def on_device(gradients, momentum, weights):
    new_weights, new_momentum = store(
        *update(to_pieces(gradients), to_pieces(momentum), to_pieces(weights))
    )
    return (from_pieces(new_weights), from_pieces(new_momentum))


def solution(mesh):
    placed = (P(None, "shard", "model"), P(None, "shard", "model"), P(None, "shard", "model"))
    return jax.shard_map(
        on_device,
        mesh=mesh,
        in_specs=placed,
        out_specs=(P(None, "shard", "model"), P(None, "shard", "model")),
        check_vma=False,
    )
```
